8 devices in a mesh: dp: 2 (over z, y), tp: 4 (over x, core).
Axes of the slice: x: 2, y: 2, z: 1, core: 2. Of those that a mesh axis runs over, the one named last changes fastest.
Arguments:
- x_chunk: bfloat16 [64, 256, 1024], P('dp', 'tp'), parts along dimension 0
- prefix_len: int32 [64], P('dp'), parts along dimension 0
- k_cache: bfloat16 [64, 2048, 16, 64], P('dp', None, 'tp'), parts along dimension 0
- v_cache: bfloat16 [64, 2048, 16, 64], P('dp', None, 'tp'), parts along dimension 0
- ln1_gain: bfloat16 [1024], replicated
- ln1_bias: bfloat16 [1024], replicated
- w_qkv: bfloat16 [1024, 3072], P(None, 'tp')
- b_qkv: bfloat16 [3072], P('tp')
- w_out: bfloat16 [1024, 1024], P('tp')
- b_out: bfloat16 [1024], replicated
- ln2_gain: bfloat16 [1024], replicated
- ln2_bias: bfloat16 [1024], replicated
- w_up: bfloat16 [1024, 4096], P(None, 'tp')
- b_up: bfloat16 [4096], P('tp')
- w_down: bfloat16 [4096, 1024], P('tp')
- b_down: bfloat16 [1024], replicated
Outputs:
- output 1: bfloat16 [64, 256, 1024], P('dp', 'tp'), parts along dimension 0
- output 2: bfloat16 [64, 2048, 16, 64], P('dp', None, 'tp'), parts along dimension 0
- output 3: bfloat16 [64, 2048, 16, 64], P('dp', None, 'tp'), parts along dimension 0
There are 2 independent parts. The reference program is written for one: setup_inputs(seed, part) draws one part's arguments, and reference() takes and returns one part's arrays. A program takes and returns all parts, laid end to end along the dimension named above; an argument that names none is the same for every part.
All inputs are finite; a program needn't handle non-finite values.
Results may differ from the reference program's by a relative error of at most 0.0118672.
Values are sent between devices in bfloat16 or wider.
A program may use at most 1 GiB of HBM per device.

```python
import jax
import jax.numpy as jnp
from jax import lax

BATCH_SEQS = 32
CHUNK_LEN = 256
CACHE_LEN = 2048
D_MODEL = 1024
NUM_HEADS = 16
HEAD_DIM = 64
FF_DIM = 4 * D_MODEL
LN_EPS = 1e-5


def setup_inputs(seed: int = 0, part: int = 0) -> dict:
    part_keys = jax.random.split(jax.random.fold_in(jax.random.key(seed), part), 5)
    shared_keys = jax.random.split(jax.random.key(seed + 7919), 12)
    max_start = CACHE_LEN - CHUNK_LEN
    starts = jax.random.randint(part_keys[1], (BATCH_SEQS,), 0, max_start + 1)
    longest = jax.random.randint(part_keys[2], (), 0, BATCH_SEQS)
    prefix_len = jnp.where(jnp.arange(BATCH_SEQS) == longest, max_start, starts).astype(jnp.int32)
    cache_shape = (BATCH_SEQS, CACHE_LEN, NUM_HEADS, HEAD_DIM)
    vec_shape = (D_MODEL,)
    d_scale = D_MODEL ** -0.5

    def normal_draw(key_in, shape_in, std_dev):
        return (std_dev * jax.random.normal(key_in, shape_in, jnp.float32)).astype(jnp.bfloat16)

    def gain_draw(key_in):
        return (1.0 + 0.25 * jax.random.normal(key_in, vec_shape, jnp.float32)).astype(jnp.bfloat16)

    return {
        'x_chunk': normal_draw(part_keys[0], (BATCH_SEQS, CHUNK_LEN, D_MODEL), 1.0),
        'prefix_len': prefix_len,
        'k_cache': normal_draw(part_keys[3], cache_shape, 1.0),
        'v_cache': normal_draw(part_keys[4], cache_shape, 1.0),
        'ln1_gain': gain_draw(shared_keys[0]),
        'ln1_bias': normal_draw(shared_keys[1], vec_shape, 0.25),
        'w_qkv': normal_draw(shared_keys[2], (D_MODEL, 3 * D_MODEL), d_scale),
        'b_qkv': normal_draw(shared_keys[3], (3 * D_MODEL,), 0.25),
        'w_out': normal_draw(shared_keys[4], (D_MODEL, D_MODEL), d_scale),
        'b_out': normal_draw(shared_keys[5], vec_shape, 0.25),
        'ln2_gain': gain_draw(shared_keys[6]),
        'ln2_bias': normal_draw(shared_keys[7], vec_shape, 0.25),
        'w_up': normal_draw(shared_keys[8], (D_MODEL, FF_DIM), d_scale),
        'b_up': normal_draw(shared_keys[9], (FF_DIM,), 0.25),
        'w_down': normal_draw(shared_keys[10], (FF_DIM, D_MODEL), FF_DIM ** -0.5),
        'b_down': normal_draw(shared_keys[11], vec_shape, 0.25),
    }


def layer_norm(tok_rows, ln_gain, ln_bias):
    rows_f32 = tok_rows.astype(jnp.float32)
    row_mean = jnp.mean(rows_f32, axis=-1, keepdims=True)
    centered = rows_f32 - row_mean
    row_var = jnp.mean(centered * centered, axis=-1, keepdims=True)
    normed = centered * lax.rsqrt(row_var + LN_EPS)
    return (normed * ln_gain.astype(jnp.float32) + ln_bias.astype(jnp.float32)).astype(jnp.bfloat16)


def write_rows(cache_seq, new_rows, start_pos):
    zero_idx = jnp.zeros_like(start_pos)
    return lax.dynamic_update_slice(cache_seq, new_rows, (start_pos, zero_idx, zero_idx))


def attend_one(operands):
    queries, keys_all, values_all, start_pos = operands
    scores = jnp.einsum('chd,thd->hct', queries.astype(jnp.float32), keys_all.astype(jnp.float32)) * (HEAD_DIM ** -0.5)
    slopes = jnp.exp2(-8.0 * (jnp.arange(NUM_HEADS) + 1).astype(jnp.float32) / NUM_HEADS)
    query_pos = start_pos + jnp.arange(CHUNK_LEN)
    rel_pos = (jnp.arange(CACHE_LEN)[None, :] - query_pos[:, None]).astype(jnp.float32)
    scores = scores + slopes[:, None, None] * rel_pos[None]
    scores = jnp.where((rel_pos <= 0.0)[None], scores, -1e30)
    attn_probs = jax.nn.softmax(scores, axis=-1).astype(jnp.bfloat16)
    context = jnp.einsum('hct,thd->chd', attn_probs.astype(jnp.float32), values_all.astype(jnp.float32))
    return context.astype(jnp.bfloat16).reshape(CHUNK_LEN, D_MODEL)


def reference(x_chunk, prefix_len, k_cache, v_cache, ln1_gain, ln1_bias, w_qkv, b_qkv, w_out, b_out, ln2_gain, ln2_bias, w_up, b_up, w_down, b_down):
    tok_rows = x_chunk.reshape(BATCH_SEQS * CHUNK_LEN, D_MODEL)
    normed = layer_norm(tok_rows, ln1_gain, ln1_bias)
    qkv_proj = jnp.dot(normed, w_qkv, preferred_element_type=jnp.float32) + b_qkv.astype(jnp.float32)
    qkv_heads = qkv_proj.astype(jnp.bfloat16).reshape(BATCH_SEQS, CHUNK_LEN, NUM_HEADS, 3, HEAD_DIM)
    k_upd = jax.vmap(write_rows)(k_cache, qkv_heads[:, :, :, 1], prefix_len)
    v_upd = jax.vmap(write_rows)(v_cache, qkv_heads[:, :, :, 2], prefix_len)
    context = lax.map(attend_one, (qkv_heads[:, :, :, 0], k_upd, v_upd, prefix_len))
    context = context.reshape(BATCH_SEQS * CHUNK_LEN, D_MODEL)
    attn_out = jnp.dot(context, w_out, preferred_element_type=jnp.float32)
    residual = (tok_rows.astype(jnp.float32) + attn_out + b_out.astype(jnp.float32)).astype(jnp.bfloat16)
    normed2 = layer_norm(residual, ln2_gain, ln2_bias)
    up_pre = jnp.dot(normed2, w_up, preferred_element_type=jnp.float32) + b_up.astype(jnp.float32)
    up_act = jax.nn.gelu(up_pre, approximate=True).astype(jnp.bfloat16)
    down_out = jnp.dot(up_act, w_down, preferred_element_type=jnp.float32)
    x_out = (residual.astype(jnp.float32) + down_out + b_down.astype(jnp.float32)).astype(jnp.bfloat16)
    return x_out.reshape(BATCH_SEQS, CHUNK_LEN, D_MODEL), k_upd, v_upd
```

```python
import functools

import jax
import jax.numpy as jnp
from jax import lax
from jax.experimental import pallas as pl
from jax.experimental.pallas import tpu as pltpu
from jax.sharding import PartitionSpec as P

LN_EPS = 1e-5
LOG2E = 1.4426950408889634
NEG = -1e30
NCHUNK = 4
KB = 256
XOR1 = [(0, 1), (1, 0), (2, 3), (3, 2)]
XOR2 = [(0, 2), (2, 0), (1, 3), (3, 1)]
XOR3 = [(0, 3), (3, 0), (1, 2), (2, 1)]
HBM = pltpu.HBM


def norm_rows(rows_f32, gain, bias):
    row_mean = jnp.mean(rows_f32, axis=-1, keepdims=True)
    centered = rows_f32 - row_mean
    row_var = jnp.mean(centered * centered, axis=-1, keepdims=True)
    normed = centered * lax.rsqrt(row_var + LN_EPS)
    return (normed * gain + bias).astype(jnp.bfloat16)


def ln_kernel(x_ref, gain_ref, bias_ref, o_ref):
    rows = x_ref[...].reshape(-1, x_ref.shape[-1]).astype(jnp.float32)
    gain = gain_ref[...].astype(jnp.float32)
    bias = bias_ref[...].astype(jnp.float32)
    o_ref[...] = norm_rows(rows, gain, bias).reshape(o_ref.shape)


def layer_norm_chunk(x, gain, bias, start, count):
    tok, dim = x.shape[1], x.shape[2]
    step = 4
    return pl.pallas_call(
        ln_kernel,
        grid=(count // step,),
        in_specs=[
            pl.BlockSpec((step, tok, dim), lambda i: (start // step + i, 0, 0)),
            pl.BlockSpec((1, dim), lambda i: (0, 0)),
            pl.BlockSpec((1, dim), lambda i: (0, 0)),
        ],
        out_specs=pl.BlockSpec((step, tok, dim), lambda i: (i, 0, 0)),
        out_shape=jax.ShapeDtypeStruct((count, tok, dim), jnp.bfloat16),
        cost_estimate=pl.CostEstimate(flops=count * tok * dim * 10, bytes_accessed=count * tok * dim * 4, transcendentals=0),
        name='ln1',
    )(x, gain, bias)


def attn_kernel(start, meta_ref, slope_ref, a0, a1, a2, a3, w_ref, b_ref, kc_ref, vc_ref, *rest):
    has_prev = start > 0
    if has_prev:
        rest = rest[2:]
    c0, c1, c2, c3, ko_ref, vo_ref, a_scr, qkv_scr, bias_scr, m_scr, acc_scr, ctx_scr = rest
    heads, hd, cache_len = kc_ref.shape[1:]
    tok = a0.shape[1]
    chunk = 4 * tok
    tp = meta_ref[0]
    step = pl.program_id(0)
    pos = meta_ref[1 + start + step]

    diff = (lax.broadcasted_iota(jnp.int32, (KB, chunk), 0) - lax.broadcasted_iota(jnp.int32, (KB, chunk), 1))

    @pl.when(step == 0)
    def _():
        for h in range(heads):
            bias_scr[h] = diff.astype(jnp.float32) * (slope_ref[h] * LOG2E)

    for k, blk in enumerate((a0, a1, a2, a3)):
        a_scr[pl.ds(pl.multiple_of((tp ^ k) * tok, tok), tok), :] = blk[0]
    qkv = lax.dot_general(w_ref[...], a_scr[...], (((1,), (1,)), ((), ())), preferred_element_type=jnp.float32)
    qkv = qkv + b_ref[...]
    qkv_scr[...] = qkv.astype(jnp.bfloat16)

    ko_ref[...] = kc_ref[...]
    vo_ref[...] = vc_ref[...]
    win = chunk + 128
    base = pl.multiple_of(jnp.minimum((pos // 128) * 128, cache_len - win), 128)
    off = pos - base
    lane = lax.broadcasted_iota(jnp.int32, (hd, win), 1)
    inside = (lane >= off) & (lane < off + chunk)
    pad = jnp.zeros((hd, 128), jnp.float32)
    for h in range(heads):
        for part, dst in ((1, ko_ref), (2, vo_ref)):
            row = h * 3 * hd + part * hd
            new = qkv_scr[row:row + hd, :].astype(jnp.float32)
            new = pltpu.roll(jnp.concatenate([new, pad], axis=1), off, 1)
            old = dst[0, h, :, pl.ds(base, win)].astype(jnp.float32)
            dst[0, h, :, pl.ds(base, win)] = jnp.where(inside, new, old).astype(jnp.bfloat16)

    m_scr[...] = jnp.full_like(m_scr, NEG)
    acc_scr[...] = jnp.zeros_like(acc_scr)
    ones = jnp.ones((16, KB), jnp.bfloat16)

    def block(kb, masked):
        j0 = pl.multiple_of(kb * KB, KB)
        for h in range(heads):
            keys = ko_ref[0, h, :, pl.ds(j0, KB)]
            vals = jnp.concatenate([vo_ref[0, h, :, pl.ds(j0, KB)], ones], axis=0)
            q = qkv_scr[h * 3 * hd:h * 3 * hd + hd, :]
            s = lax.dot_general(keys, q, (((0,), (0,)), ((), ())), preferred_element_type=jnp.float32)
            s = s * (LOG2E * hd ** -0.5) + bias_scr[h]
            if masked:
                s = jnp.where(diff <= pos - j0, s, NEG)
            shift = slope_ref[h] * LOG2E * (j0 - pos).astype(jnp.float32)
            m_old = m_scr[h]
            m_new = jnp.maximum(m_old, jnp.max(s, axis=0, keepdims=True) + shift)
            p = jnp.exp2(s - (m_new - shift)).astype(jnp.bfloat16)
            alpha = jnp.exp2(m_old - m_new)
            m_scr[h] = m_new
            acc_scr[h] = acc_scr[h] * alpha + jnp.dot(vals, p, preferred_element_type=jnp.float32)

    full = pos // KB
    total = (pos + chunk + KB - 1) // KB
    lax.fori_loop(0, full, lambda kb, c: (block(kb, False), c)[1], 0)
    lax.fori_loop(full, total, lambda kb, c: (block(kb, True), c)[1], 0)

    for h in range(heads):
        ctx = acc_scr[h, :hd, :] / acc_scr[h, hd:hd + 1, :]
        ctx_scr[:, h * hd:(h + 1) * hd] = ctx.T.astype(jnp.bfloat16)
    for k, out in enumerate((c0, c1, c2, c3)):
        out[0] = ctx_scr[pl.ds(pl.multiple_of((tp ^ k) * tok, tok), tok), :]


def attention_chunk(meta, slopes, blocks, w_t, b_col, k_t, v_t, prev, start):
    count, tok, dim = blocks[0].shape
    heads, hd, cache_len = k_t.shape[1:]
    chunk = 4 * tok
    cols = heads * hd
    tok_spec = pl.BlockSpec((1, tok, dim), lambda i, *_: (i, 0, 0))
    cache_spec = pl.BlockSpec((1, heads, hd, cache_len), lambda i, *_: (start + i, 0, 0, 0))
    any_spec = pl.BlockSpec(memory_space=pl.ANY)
    in_specs = [tok_spec] * 4 + [
        pl.BlockSpec(w_t.shape, lambda i, *_: (0, 0)),
        pl.BlockSpec(b_col.shape, lambda i, *_: (0, 0)),
        cache_spec, cache_spec]
    operands = [*blocks, w_t, b_col, k_t, v_t]
    aliases = {}
    if prev is not None:
        in_specs += [any_spec, any_spec]
        operands += list(prev)
        aliases = {2 + 8: 4, 2 + 9: 5}
    ctx_spec = pl.BlockSpec((1, tok, cols), lambda i, *_: (i, 0, 0))
    return pl.pallas_call(
        functools.partial(attn_kernel, start),
        grid_spec=pltpu.PrefetchScalarGridSpec(
            num_scalar_prefetch=2,
            grid=(count,),
            in_specs=in_specs,
            out_specs=[ctx_spec] * 4 + [cache_spec, cache_spec],
            scratch_shapes=[
                pltpu.VMEM((chunk, dim), jnp.bfloat16),
                pltpu.VMEM((3 * cols, chunk), jnp.bfloat16),
                pltpu.VMEM((heads, KB, chunk), jnp.float32),
                pltpu.VMEM((heads, 1, chunk), jnp.float32),
                pltpu.VMEM((heads, hd + 16, chunk), jnp.float32),
                pltpu.VMEM((chunk, cols), jnp.bfloat16),
            ]),
        out_shape=[jax.ShapeDtypeStruct((count, tok, cols), jnp.bfloat16)] * 4
        + [jax.ShapeDtypeStruct(k_t.shape, k_t.dtype)] * 2,
        input_output_aliases=aliases,
        cost_estimate=pl.CostEstimate(
            flops=count * 20 * 500_000_000, bytes_accessed=count * 4 * heads * hd * cache_len * 2, transcendentals=0),
        compiler_params=pltpu.CompilerParams(vmem_limit_bytes=40 * 1024 * 1024),
        name='attn',
    )(meta, slopes, *operands)


def mlp_kernel(start, rows, *refs):
    c0, c1, c2, c3, x_ref, bo_ref, g2_ref, b2_ref, bu0, bu1, bu2, bu3, bd_ref = refs[:13]
    wo_hbm = refs[13:17]
    wu_hbm = refs[17:21]
    wd_hbm = refs[21:25]
    rest = refs[25:]
    if start > 0:
        rest = rest[1:]
    o_ref, wo, wu, wd, sem_o, sem_u, sem_d, n_scr, r_scr, h_scr, y_scr = rest
    dim = x_ref.shape[-1]

    def copies(k):
        return (pltpu.make_async_copy(wo_hbm[k], wo.at[k], sem_o.at[k]),
                pltpu.make_async_copy(wu_hbm[k], wu.at[k], sem_u.at[k]),
                pltpu.make_async_copy(wd_hbm[k], wd.at[k], sem_d.at[k]))

    for k in range(4):
        copies(k)[0].start()
    for k in range(4):
        copies(k)[1].start()
        copies(k)[2].start()

    y = None
    for k, c in enumerate((c0, c1, c2, c3)):
        copies(k)[0].wait()
        part = jnp.dot(c[...].reshape(rows, -1), wo[k], preferred_element_type=jnp.float32)
        y = part if y is None else y + part
    r = (x_ref[...].reshape(rows, dim).astype(jnp.float32) + y + bo_ref[...].astype(jnp.float32)).astype(jnp.bfloat16)
    r_scr[...] = r
    n_scr[...] = norm_rows(r.astype(jnp.float32), g2_ref[...].astype(jnp.float32), b2_ref[...].astype(jnp.float32))
    for k, bu in enumerate((bu0, bu1, bu2, bu3)):
        copies(k)[1].wait()
        copies(k)[2].wait()
        up = jnp.dot(n_scr[...], wu[k], preferred_element_type=jnp.float32) + bu[...].astype(jnp.float32)
        h_scr[...] = jax.nn.gelu(up, approximate=True).astype(jnp.bfloat16)
        down = jnp.dot(h_scr[...], wd[k], preferred_element_type=jnp.float32)
        if k == 0:
            y_scr[...] = down
        elif k < 3:
            y_scr[...] += down
        else:
            out = r_scr[...].astype(jnp.float32) + (y_scr[...] + down) + bd_ref[...].astype(jnp.float32)
            o_ref[...] = out.astype(jnp.bfloat16).reshape(o_ref.shape)


def mlp_chunk(ctx, x, small, wo, wu, wd, prev, start):
    count, tok, cols = ctx[0].shape
    dim = x.shape[2]
    rows = count * tok
    hid = wu[0].shape[1]
    whole = lambda a: pl.BlockSpec(a.shape, lambda i: (0,) * a.ndim)
    any_spec = pl.BlockSpec(memory_space=pl.ANY)
    x_spec = pl.BlockSpec((count, tok, dim), lambda i: (start // count, 0, 0))
    in_specs = [whole(c) for c in ctx] + [x_spec] + [whole(a) for a in small] + [any_spec] * 12
    operands = [*ctx, x, *small, *wo, *wu, *wd]
    aliases = {}
    if prev is not None:
        aliases = {len(operands): 0}
        in_specs.append(any_spec)
        operands.append(prev)
    return pl.pallas_call(
        functools.partial(mlp_kernel, start, rows),
        grid=(1,),
        in_specs=in_specs,
        out_specs=x_spec,
        out_shape=jax.ShapeDtypeStruct(x.shape, x.dtype),
        scratch_shapes=[
            pltpu.VMEM((4, cols, dim), jnp.bfloat16),
            pltpu.VMEM((4, dim, hid), jnp.bfloat16),
            pltpu.VMEM((4, hid, dim), jnp.bfloat16),
            pltpu.SemaphoreType.DMA((4,)),
            pltpu.SemaphoreType.DMA((4,)),
            pltpu.SemaphoreType.DMA((4,)),
            pltpu.VMEM((rows, dim), jnp.bfloat16),
            pltpu.VMEM((rows, dim), jnp.bfloat16),
            pltpu.VMEM((rows, hid), jnp.bfloat16),
            pltpu.VMEM((rows, dim), jnp.float32),
        ],
        input_output_aliases=aliases,
        cost_estimate=pl.CostEstimate(
            flops=20 * rows * 9 * dim * dim * 2, bytes_accessed=rows * dim * 8 + 18 * dim * dim, transcendentals=0),
        compiler_params=pltpu.CompilerParams(vmem_limit_bytes=52 * 1024 * 1024),
        name='mlp',
    )(*operands)


def solution(mesh):
    tp_size = mesh.shape['tp']

    def local_layer(x, prefix_len, k_cache, v_cache, ln1_gain, ln1_bias, w_qkv, b_qkv, w_out, b_out, ln2_gain, ln2_bias, w_up, b_up, w_down, b_down):
        batch = x.shape[0]
        heads = k_cache.shape[2]
        count = batch // NCHUNK
        tp = lax.axis_index('tp')
        row = lambda a: a.reshape(1, -1)
        perm = lambda a, pairs: lax.ppermute(a, 'tp', pairs)

        def gather(a):
            near, far = perm(a, XOR1), perm(a, XOR2)
            return [a, near, far, perm(far, XOR1)]

        normed = [layer_norm_chunk(x, row(ln1_gain), row(ln1_bias), c * count, count) for c in range(NCHUNK)]
        blocks = [gather(n) for n in normed]
        wo, wu, wd, bu = gather(w_out), gather(w_up), gather(w_down), gather(row(b_up))

        meta = jnp.concatenate([tp[None].astype(jnp.int32), prefix_len])
        head_ids = tp * heads + jnp.arange(heads)
        slopes = jnp.exp2(-8.0 * (head_ids + 1).astype(jnp.float32) / (heads * tp_size))
        w_t = w_qkv.T
        b_col = b_qkv.astype(jnp.float32).reshape(-1, 1)
        k_t = k_cache.transpose(0, 2, 3, 1)
        v_t = v_cache.transpose(0, 2, 3, 1)
        small = [row(b_out), row(ln2_gain), row(ln2_bias), *bu, row(b_down)]

        caches, x_out = None, None
        sent = []
        for c in range(NCHUNK):
            outs = attention_chunk(meta, slopes, blocks[c], w_t, b_col, k_t, v_t, caches, c * count)
            caches = outs[4:]
            sent.append([outs[0], perm(outs[1], XOR1), perm(outs[2], XOR2), perm(outs[3], XOR3)])
        for c in range(NCHUNK):
            x_out = mlp_chunk(sent[c], x, small, wo, wu, wd, x_out, c * count)
        return x_out, caches[0].transpose(0, 3, 1, 2), caches[1].transpose(0, 3, 1, 2)

    tok_spec = P('dp', 'tp', None)
    cache_spec = P('dp', None, 'tp', None)
    replicated = P()
    in_specs = (tok_spec, P('dp'), cache_spec, cache_spec, replicated, replicated, P(None, 'tp'), P('tp'), P('tp', None), replicated, replicated, replicated, P(None, 'tp'), P('tp'), P('tp', None), replicated)
    return jax.shard_map(local_layer, mesh=mesh, in_specs=in_specs, out_specs=(tok_spec, cache_spec, cache_spec), check_vma=False)
```

```python
import functools

import jax
import jax.numpy as jnp
from jax import lax
from jax.experimental import pallas as pl
from jax.experimental.pallas import tpu as pltpu
from jax.sharding import PartitionSpec as P


LN_EPS = 1e-5
LOG2E = 1.4426950408889634
NEG = -1e30
CHUNKS = (4, 4, 8, 8, 8)
GROUPS = ((0, 1), (2,), (3,), (4,))
KB = 256
XOR1 = [(0, 1), (1, 0), (2, 3), (3, 2)]
XOR2 = [(0, 2), (2, 0), (1, 3), (3, 1)]
XOR3 = [(0, 3), (3, 0), (1, 2), (2, 1)]


def norm_rows(rows_f32, gain, bias):
    row_mean = jnp.mean(rows_f32, axis=-1, keepdims=True)
    centered = rows_f32 - row_mean
    row_var = jnp.mean(centered * centered, axis=-1, keepdims=True)
    normed = centered * lax.rsqrt(row_var + LN_EPS)
    return (normed * gain + bias).astype(jnp.bfloat16)


def ln_kernel(x_ref, gain_ref, bias_ref, o_ref):
    rows = x_ref[...].reshape(-1, x_ref.shape[-1]).astype(jnp.float32)
    gain = gain_ref[...].astype(jnp.float32)
    bias = bias_ref[...].astype(jnp.float32)
    o_ref[...] = norm_rows(rows, gain, bias).reshape(o_ref.shape)


def layer_norm_chunk(x, gain, bias, start, count):
    tok, dim = x.shape[1], x.shape[2]
    step = 4
    return pl.pallas_call(
        ln_kernel,
        grid=(count // step,),
        in_specs=[
            pl.BlockSpec((step, tok, dim), lambda i: (start // step + i, 0, 0)),
            pl.BlockSpec((1, dim), lambda i: (0, 0)),
            pl.BlockSpec((1, dim), lambda i: (0, 0)),
        ],
        out_specs=pl.BlockSpec((step, tok, dim), lambda i: (i, 0, 0)),
        out_shape=jax.ShapeDtypeStruct((count, tok, dim), jnp.bfloat16),
        cost_estimate=pl.CostEstimate(flops=count * tok * dim * 10, bytes_accessed=count * tok * dim * 4, transcendentals=0),
        name='ln1',
    )(x, gain, bias)


def attn_kernel(start, meta_ref, slope_ref, a0, a1, a2, a3, w_ref, b_ref, kc_ref, vc_ref, *rest):
    has_prev = start > 0
    if has_prev:
        rest = rest[2:]
    c0, c1, c2, c3, ko_ref, vo_ref, a_scr, qkv_scr, bias_scr, m_scr, acc_scr, ctx_scr, s_scr, top_scr = rest
    heads, hd, cache_len = kc_ref.shape[1:]
    tok = a0.shape[1]
    chunk = 4 * tok
    tp = meta_ref[0]
    step = pl.program_id(0)
    pos = meta_ref[1 + start + step]

    diff = (lax.broadcasted_iota(jnp.int32, (KB, chunk), 0) - lax.broadcasted_iota(jnp.int32, (KB, chunk), 1))

    @pl.when(step == 0)
    def _():
        for h in range(heads):
            bias_scr[h] = diff.astype(jnp.float32) * (slope_ref[h] * LOG2E)

    for k, blk in enumerate((a0, a1, a2, a3)):
        a_scr[pl.ds(pl.multiple_of((tp ^ k) * tok, tok), tok), :] = blk[0]
    qkv = lax.dot_general(w_ref[...], a_scr[...], (((1,), (1,)), ((), ())), preferred_element_type=jnp.float32)
    qkv = qkv + b_ref[...]
    qkv_scr[...] = qkv.astype(jnp.bfloat16)

    ko_ref[...] = kc_ref[...]
    vo_ref[...] = vc_ref[...]
    win = chunk + 128
    base = pl.multiple_of(jnp.minimum((pos // 128) * 128, cache_len - win), 128)
    off = pos - base
    lane = lax.broadcasted_iota(jnp.int32, (hd, win), 1)
    inside = (lane >= off) & (lane < off + chunk)
    pad = jnp.zeros((hd, 128), jnp.float32)
    for h in range(heads):
        for part, dst in ((1, ko_ref), (2, vo_ref)):
            row = h * 3 * hd + part * hd
            new = qkv_scr[row:row + hd, :].astype(jnp.float32)
            new = pltpu.roll(jnp.concatenate([new, pad], axis=1), off, 1)
            old = dst[0, h, :, pl.ds(base, win)].astype(jnp.float32)
            dst[0, h, :, pl.ds(base, win)] = jnp.where(inside, new, old).astype(jnp.bfloat16)

    m_scr[...] = jnp.full_like(m_scr, NEG)
    acc_scr[...] = jnp.zeros_like(acc_scr)
    ones = jnp.ones((16, KB), jnp.bfloat16)

    def raw_scores(h, kb):
        keys = ko_ref[0, h, :, pl.ds(pl.multiple_of(kb * KB, KB), KB)]
        q = qkv_scr[h * 3 * hd:h * 3 * hd + hd, :]
        return lax.dot_general(keys, q, (((0,), (0,)), ((), ())), preferred_element_type=jnp.float32)

    def keep_scores(h, kb, s, masked):
        bias = bias_scr[h]
        s = s * (LOG2E * hd ** -0.5) + bias
        if masked:
            bound = (pos - kb * KB).astype(jnp.float32) * (slope_ref[h] * LOG2E)
            s = jnp.where(bias <= bound, s, NEG)
        s_scr[h] = s
        top_scr[h] = jnp.max(s, axis=0, keepdims=True)

    def weigh(h, kb):
        j0 = pl.multiple_of(kb * KB, KB)
        vals = jnp.concatenate([vo_ref[0, h, :, pl.ds(j0, KB)], ones], axis=0)
        shift = slope_ref[h] * LOG2E * (j0 - pos).astype(jnp.float32)
        m_old = m_scr[h]
        m_new = jnp.maximum(m_old, top_scr[h] + shift)
        p = jnp.exp2(s_scr[h] - (m_new - shift)).astype(jnp.bfloat16)
        alpha = jnp.exp2(m_old - m_new)
        m_scr[h] = m_new
        acc_scr[h] = acc_scr[h] * alpha + jnp.dot(vals, p, preferred_element_type=jnp.float32)

    def both(kb, masked):
        for h in range(heads):
            s = raw_scores(h, kb + 1)
            weigh(h, kb)
            keep_scores(h, kb + 1, s, masked)

    full = pos // KB
    total = (pos + chunk + KB - 1) // KB
    first = [raw_scores(h, 0) for h in range(heads)]
    for h in range(heads):
        keep_scores(h, 0, first[h], True)
    split = jnp.maximum(full - 1, 0)
    lax.fori_loop(0, split, lambda kb, c: (both(kb, False), c)[1], 0)
    lax.fori_loop(split, total - 1, lambda kb, c: (both(kb, True), c)[1], 0)
    for h in range(heads):
        weigh(h, total - 1)

    for h in range(heads):
        ctx = acc_scr[h, :hd, :] / acc_scr[h, hd:hd + 1, :]
        ctx_scr[:, h * hd:(h + 1) * hd] = ctx.T.astype(jnp.bfloat16)
    for k, out in enumerate((c0, c1, c2, c3)):
        out[0] = ctx_scr[pl.ds(pl.multiple_of((tp ^ k) * tok, tok), tok), :]


def attention_chunk(meta, slopes, blocks, w_t, b_col, k_t, v_t, prev, start):
    count, tok, dim = blocks[0].shape
    heads, hd, cache_len = k_t.shape[1:]
    chunk = 4 * tok
    cols = heads * hd
    tok_spec = pl.BlockSpec((1, tok, dim), lambda i, *_: (i, 0, 0))
    cache_spec = pl.BlockSpec((1, heads, hd, cache_len), lambda i, *_: (start + i, 0, 0, 0))
    any_spec = pl.BlockSpec(memory_space=pl.ANY)
    in_specs = [tok_spec] * 4 + [
        pl.BlockSpec(w_t.shape, lambda i, *_: (0, 0)),
        pl.BlockSpec(b_col.shape, lambda i, *_: (0, 0)),
        cache_spec, cache_spec]
    operands = [*blocks, w_t, b_col, k_t, v_t]
    aliases = {}
    if prev is not None:
        in_specs += [any_spec, any_spec]
        operands += list(prev)
        aliases = {2 + 8: 4, 2 + 9: 5}
    ctx_spec = pl.BlockSpec((1, tok, cols), lambda i, *_: (i, 0, 0))
    return pl.pallas_call(
        functools.partial(attn_kernel, start),
        grid_spec=pltpu.PrefetchScalarGridSpec(
            num_scalar_prefetch=2,
            grid=(count,),
            in_specs=in_specs,
            out_specs=[ctx_spec] * 4 + [cache_spec, cache_spec],
            scratch_shapes=[
                pltpu.VMEM((chunk, dim), jnp.bfloat16),
                pltpu.VMEM((3 * cols, chunk), jnp.bfloat16),
                pltpu.VMEM((heads, KB, chunk), jnp.float32),
                pltpu.VMEM((heads, 1, chunk), jnp.float32),
                pltpu.VMEM((heads, hd + 16, chunk), jnp.float32),
                pltpu.VMEM((chunk, cols), jnp.bfloat16),
                pltpu.VMEM((heads, KB, chunk), jnp.float32),
                pltpu.VMEM((heads, 1, chunk), jnp.float32),
            ]),
        out_shape=[jax.ShapeDtypeStruct((count, tok, cols), jnp.bfloat16)] * 4
        + [jax.ShapeDtypeStruct(k_t.shape, k_t.dtype)] * 2,
        input_output_aliases=aliases,
        cost_estimate=pl.CostEstimate(
            flops=count * 3_000_000_000, bytes_accessed=count * 4 * heads * hd * cache_len * 2, transcendentals=0),
        compiler_params=pltpu.CompilerParams(vmem_limit_bytes=40 * 1024 * 1024),
        name='attn',
    )(meta, slopes, *operands)


def mlp_kernel(nsub, half_ref, *refs):
    ctx_refs = refs[:4 * nsub]
    x_ref, bo_ref, g2_ref, b2_ref, bd_ref = refs[4 * nsub:4 * nsub + 5]
    packs = refs[4 * nsub + 5:4 * nsub + 17]
    o_ref, wu, wd, wo, bu, ctx_scr, n_scr, r_scr, h_scr, y_scr, sem_a, sem_b, sem_o, sem_u = refs[-14:]
    rows, dim = n_scr.shape
    hid = wd.shape[1]
    tok = x_ref.shape[1]
    cut = wo.shape[0] // 8

    def copies(j):
        pa, pb = (packs[0].at[j], packs[1].at[j]) if j < 2 else (packs[2].at[j - 2], packs[3].at[j - 2]) if j < 4 else (packs[2 * j - 4], packs[2 * j - 3])
        return (pltpu.make_async_copy(pa.at[pl.ds(hid, cut), :], wo.at[pl.ds(j * cut, cut), :], sem_o.at[j]),
                pltpu.make_async_copy(pa.at[pl.ds(hid + cut, 16), :], bu.at[j], sem_u.at[j]),
                pltpu.make_async_copy(pa.at[pl.ds(0, hid), :], wu.at[j], sem_a.at[j]),
                pltpu.make_async_copy(pb, wd.at[j], sem_b.at[j]))

    for part in (0, 1):
        for j in range(8):
            copies(j)[part].start()
    for j in range(8):
        copies(j)[2].start()
        copies(j)[3].start()

    half = half_ref[0]
    for i in range(nsub):
        size = ctx_refs[4 * i].shape[0] * tok
        for k in range(4):
            for side in (0, 1):
                pick = half if side == 0 else 1 - half
                at = side * cut if k < 2 else pl.multiple_of(pick * cut, cut)
                piece = ctx_refs[4 * i + k][:, :, pl.ds(at, cut)].reshape(size, cut)
                ctx_scr[i * size:(i + 1) * size, (2 * k + side) * cut:(2 * k + side + 1) * cut] = piece
    for j in range(8):
        copies(j)[0].wait()
        copies(j)[1].wait()

    y = jnp.dot(ctx_scr[...], wo[...], preferred_element_type=jnp.float32)
    r = (x_ref[...].reshape(rows, dim).astype(jnp.float32) + y + bo_ref[...].astype(jnp.float32)).astype(jnp.bfloat16)
    r_scr[...] = r
    n_scr[...] = norm_rows(r.astype(jnp.float32), g2_ref[...].astype(jnp.float32), b2_ref[...].astype(jnp.float32))
    y_scr[...] = jnp.zeros_like(y_scr)
    lim = 256

    def wait_pack(j):
        pltpu.make_async_copy(packs[1].at[0], wu.at[j], sem_a.at[j]).wait()
        pltpu.make_async_copy(packs[1].at[0], wd.at[j], sem_b.at[j]).wait()

    def up(m, j):
        return (jnp.dot(n_scr[m:m + lim, :hid], wu[j, :, :hid], preferred_element_type=jnp.float32)
                + jnp.dot(n_scr[m:m + lim, hid:], wu[j, :, hid:], preferred_element_type=jnp.float32))

    def act(m, j, pre):
        h_scr[m:m + lim, :] = jax.nn.gelu(pre + bu[j, 0:1, :hid].astype(jnp.float32), approximate=True).astype(jnp.bfloat16)

    def down(m, j):
        y_scr[m:m + lim, :] += jnp.dot(h_scr[m:m + lim, :], wd[j], preferred_element_type=jnp.float32)

    steps = range(0, rows, lim)
    wait_pack(0)
    pre = [up(m, 0) for m in steps]
    for m, p in zip(steps, pre):
        act(m, 0, p)

    def body(j, c):
        wait_pack(j + 1)
        pre = [up(m, j + 1) for m in steps]
        for m, p in zip(steps, pre):
            down(m, j)
            act(m, j + 1, p)
        return c

    lax.fori_loop(0, 7, body, 0)
    for m in steps:
        down(m, 7)
    out = r_scr[...].astype(jnp.float32) + y_scr[...] + bd_ref[...].astype(jnp.float32)
    o_ref[...] = out.astype(jnp.bfloat16).reshape(o_ref.shape)


def mlp_chunk(half, ctx, x, small, packs, prev, start, count):
    tok, cols = ctx[0].shape[1:]
    dim = x.shape[2]
    rows = count * tok
    hid = packs[1].shape[1]
    whole = lambda a: pl.BlockSpec(a.shape, lambda i, *_: (0,) * a.ndim)
    any_spec = pl.BlockSpec(memory_space=pl.ANY)
    x_spec = pl.BlockSpec((count, tok, dim), lambda i, *_: (start // count, 0, 0))
    in_specs = [whole(c) for c in ctx] + [x_spec] + [whole(a) for a in small] + [any_spec] * 12
    operands = [half, *ctx, x, *small, *packs]
    aliases = {}
    if prev is not None:
        aliases = {len(operands): 0}
        in_specs.append(any_spec)
        operands.append(prev)
    return pl.pallas_call(
        functools.partial(mlp_kernel, len(ctx) // 4),
        grid_spec=pltpu.PrefetchScalarGridSpec(
            num_scalar_prefetch=1,
            grid=(1,),
            in_specs=in_specs,
            out_specs=x_spec,
            scratch_shapes=[
                pltpu.VMEM((8, hid, dim), jnp.bfloat16),
                pltpu.VMEM((8, hid, dim), jnp.bfloat16),
                pltpu.VMEM((4 * cols, dim), jnp.bfloat16),
                pltpu.VMEM((8, 16, dim), jnp.bfloat16),
                pltpu.VMEM((rows, 4 * cols), jnp.bfloat16),
                pltpu.VMEM((rows, dim), jnp.bfloat16),
                pltpu.VMEM((rows, dim), jnp.bfloat16),
                pltpu.VMEM((rows, hid), jnp.bfloat16),
                pltpu.VMEM((rows, dim), jnp.float32),
                pltpu.SemaphoreType.DMA((8,)),
                pltpu.SemaphoreType.DMA((8,)),
                pltpu.SemaphoreType.DMA((8,)),
                pltpu.SemaphoreType.DMA((8,)),
            ]),
        out_shape=jax.ShapeDtypeStruct(x.shape, x.dtype),
        input_output_aliases=aliases,
        cost_estimate=pl.CostEstimate(
            flops=rows * 9 * dim * dim * 2, bytes_accessed=rows * dim * 8 + 18 * dim * dim, transcendentals=0),
        compiler_params=pltpu.CompilerParams(vmem_limit_bytes=52 * 1024 * 1024),
        name='mlp',
    )(*operands)


def solution(mesh):
    tp_size = mesh.shape['tp']

    def local_layer(x, prefix_len, k_cache, v_cache, ln1_gain, ln1_bias, w_qkv, b_qkv, w_out, b_out, ln2_gain, ln2_bias, w_up, b_up, w_down, b_down):
        heads = k_cache.shape[2]
        dim = x.shape[2]
        tp = lax.axis_index('tp')
        dp = lax.axis_index('dp')
        row = lambda a: a.reshape(1, -1)

        def perm(a, pairs, axis='tp'):
            return lax.ppermute(a, axis, pairs)

        def gather(a):
            far = perm(a, XOR2)
            return [a, perm(a, XOR1), far, perm(far, XOR1)]

        starts = [sum(CHUNKS[:c]) for c in range(len(CHUNKS))]
        normed = []
        for c, s in enumerate(starts):
            normed.append(layer_norm_chunk(x, row(ln1_gain), row(ln1_bias), s, CHUNKS[c]))
        blocks = [gather(n) for n in normed]

        half = w_up.shape[1] // 2
        cut = w_out.shape[0] // 2
        pad = jnp.zeros((15, dim), jnp.bfloat16)
        pack_a, pack_b = [], []
        for i in range(2):
            up = w_up[:, i * half:(i + 1) * half]
            bias = jnp.concatenate([row(b_up)[:, i * half:(i + 1) * half], pad[:1, :dim - half]], axis=1)
            pack_a.append(jnp.concatenate([
                jnp.concatenate([up[:half], up[half:]], axis=1), w_out[i * cut:(i + 1) * cut], bias, pad], axis=0))
            pack_b.append(w_down[i * half:(i + 1) * half])
        pack_a, pack_b = jnp.stack(pack_a), jnp.stack(pack_b)
        packs = [pack_a, pack_b, perm(pack_a, XOR1), perm(pack_b, XOR1)]
        far = []
        for pack in (pack_a, pack_b):
            mine = lax.dynamic_index_in_dim(pack, dp, 0, keepdims=False)
            direct = perm(mine, XOR2)
            side = perm(direct, [(0, 1), (1, 0)], 'dp')
            far.append((direct, side, perm(direct, XOR1), perm(side, XOR1)))
        for k in range(4):
            packs += [far[0][k], far[1][k]]

        meta = jnp.concatenate([tp[None].astype(jnp.int32), prefix_len])
        head_ids = tp * heads + jnp.arange(heads)
        slopes = jnp.exp2(-8.0 * (head_ids + 1).astype(jnp.float32) / (heads * tp_size))
        w_t = w_qkv.T
        b_col = b_qkv.astype(jnp.float32).reshape(-1, 1)
        k_t = k_cache.transpose(0, 2, 3, 1)
        v_t = v_cache.transpose(0, 2, 3, 1)
        small = [row(b_out), row(ln2_gain), row(ln2_bias), row(b_down)]
        my_half = dp[None].astype(jnp.int32)

        caches, x_out = None, None
        sent = []
        for c, s in enumerate(starts):
            outs = attention_chunk(meta, slopes, blocks[c], w_t, b_col, k_t, v_t, caches, s)
            caches = outs[4:]
            sent.append([outs[0], perm(outs[1], XOR1), perm(outs[2], XOR2), perm(outs[3], XOR3)])
        for g in GROUPS:
            s, n = starts[g[0]], sum(CHUNKS[c] for c in g)
            ctx = sum((sent[c] for c in g), [])
            x_out = mlp_chunk(my_half, ctx, x, small, packs, x_out, s, n)
        return x_out, caches[0].transpose(0, 3, 1, 2), caches[1].transpose(0, 3, 1, 2)

    tok_spec = P('dp', 'tp', None)
    cache_spec = P('dp', None, 'tp', None)
    replicated = P()
    in_specs = (tok_spec, P('dp'), cache_spec, cache_spec, replicated, replicated, P(None, 'tp'), P('tp'), P('tp', None), replicated, replicated, replicated, P(None, 'tp'), P('tp'), P('tp', None), replicated)

    return jax.shard_map(local_layer, mesh=mesh, in_specs=in_specs, out_specs=(tok_spec, cache_spec, cache_spec), check_vma=False)
```
